256 devices in a mesh: rows: 64 (over x, z, core), grp: 4 (over y).
Axes of the slice: x: 4, y: 4, z: 8, core: 2. Of those that a mesh axis runs over, the one named last changes fastest.
Arguments:
- matrix: bfloat16 [81920, 16384], P(('rows', 'grp')), may hold values from -36 to 36
- sample_rows: int32 [256, 128, 256], P(('rows', 'grp')), may hold values from 0 to 319
- pair_list: int32 [64, 64, 4], replicated, may hold values from 0 to 2047, as said below
- pair_count: int32 [64, 64], replicated, may hold values from 1 to 4, as said below
- pair_blocks: int32 [2048, 2], replicated, may hold values from 0 to 127, as said below
Outputs:
- gram: float32 [2048, 128, 128], P(('rows', 'grp'))
The draws below stay inside these ranges and needn't reach their ends.
Inputs may be any that keep to these rules, and one draw needn't show every extreme that they name: `pair_list`: entry [s, r, k] lies in [r * 32, (r + 1) * 32); the 4 entries of one [s, r] are distinct. `pair_count`: every row group has some owner with all 4 slots active, and some owner has all 4 slots active from every row group. `pair_blocks`: the two blocks of a pair differ.
All inputs are finite; a program needn't handle non-finite values.
Results may differ from the reference program's by a relative error of at most 0.0016.
Values sent between devices are 32-bit elements; how exact they have to be, the bound alone decides.
A program may use at most 192 MiB of HBM per device.

```python
import math
import jax
import jax.numpy as jnp
from jax import lax

BLOCK = 128
NB = 128
ROWS_DEV = 320
SAMP = 256
CAP = 4
NCOL = 16384
ROWS_TOTAL = 81920
PAIRS = 2048
REGION = 32
N_ROWS = 64
N_GRP = 4
DEVICES = 256


def draw_matrix(key, part):
    key_base, key_row, key_col = jax.random.split(key, 3)
    row_scale = jnp.exp(jax.random.uniform(key_row, (ROWS_TOTAL, 1), jnp.float32, math.log(0.3), math.log(3.0)))
    col_scale = jnp.exp(jax.random.uniform(key_col, (1, NCOL), jnp.float32, math.log(0.5), math.log(2.0)))
    base = jnp.clip(jax.random.normal(key_base, (ROWS_TOTAL, NCOL), jnp.float32), -6.0, 6.0)
    return (base * row_scale * col_scale).astype(jnp.bfloat16)


def draw_pair_list(key, part):
    keys = jax.random.split(jax.random.fold_in(key, 11), N_ROWS * N_ROWS)
    chosen = jax.vmap(lambda single: jax.random.permutation(single, REGION)[:CAP])(keys)
    chosen = chosen.reshape(N_ROWS, N_ROWS, CAP).astype(jnp.int32)
    owner_base = (jnp.arange(N_ROWS, dtype=jnp.int32) * REGION)[None, :, None]
    return chosen + owner_base


def draw_pair_count(key, part):
    key_count, key_row, key_col = jax.random.split(jax.random.fold_in(key, 23), 3)
    counts = jax.random.randint(key_count, (N_ROWS, N_ROWS), 1, CAP + 1).astype(jnp.int32)
    full_owner = jax.random.randint(key_row, (N_ROWS,), 0, N_ROWS)
    counts = counts.at[jnp.arange(N_ROWS), full_owner].set(CAP)
    common_owner = jax.random.randint(key_col, (), 0, N_ROWS)
    counts = counts.at[:, common_owner].set(CAP)
    return counts.astype(jnp.int32)


def draw_pair_blocks(key, part):
    key_first, key_step = jax.random.split(jax.random.fold_in(key, 37))
    first_block = jax.random.randint(key_first, (PAIRS,), 0, NB)
    step_size = jax.random.randint(key_step, (PAIRS,), 1, NB)
    second_block = (first_block + step_size) % NB
    return jnp.stack([first_block, second_block], axis=1).astype(jnp.int32)


def touch_ends(result, rng, smallest, high):
    dims = result.shape
    place = [jax.random.randint(jax.random.fold_in(rng, axis), (), 0, dims[axis]) for axis in range(len(dims))]
    result = result.at[tuple(place)].set(smallest)
    longest = dims.index(max(dims))
    place[longest] = (place[longest] + 1) % dims[longest]
    return result.at[tuple(place)].set(high)


def setup_inputs(seed: int = 0) -> dict:
    seeds = jax.random.split(jax.random.key(seed), 6)
    return {
        "matrix": draw_matrix(jax.random.fold_in(seeds[5], 71), 0),
        "sample_rows": touch_ends(jax.random.randint(seeds[1], (DEVICES, NB, SAMP), 0, ROWS_DEV), jax.random.fold_in(seeds[1], 1), 0, ROWS_DEV - 1).astype(jnp.int32),
        "pair_list": draw_pair_list(jax.random.fold_in(seeds[5], 71), 0),
        "pair_count": draw_pair_count(jax.random.fold_in(seeds[5], 71), 0),
        "pair_blocks": draw_pair_blocks(jax.random.fold_in(seeds[5], 71), 0),
    }


def reference(matrix, sample_rows, pair_list, pair_count, pair_blocks):
    device_total = N_ROWS * N_GRP
    blocks_all = matrix.reshape(device_total, ROWS_DEV, NB, BLOCK)
    positions = jnp.arange(ROWS_DEV, dtype=jnp.int32)
    slot_numbers = jnp.arange(CAP, dtype=jnp.int32)

    def one_device(raw_tiles, device):
        source = device // N_GRP
        blocks = blocks_all[device]
        picked = sample_rows[device]
        multiplicity = lax.optimization_barrier(jnp.sum((picked[:, :, None] == positions[None, None, :]).astype(jnp.float32), axis=1))
        weighted = (jnp.transpose(multiplicity)[:, :, None] * blocks.astype(jnp.float32)).astype(jnp.bfloat16)
        pair_ids = pair_list[source].reshape(-1)
        live_mask = (slot_numbers[None, :] < pair_count[source][:, None]).reshape(-1).astype(jnp.float32)
        first_block = pair_blocks[pair_ids, 0]
        second_block = pair_blocks[pair_ids, 1]
        weighted_cols = jnp.take(weighted, first_block, axis=1).astype(jnp.float32)
        plain_cols = jnp.take(blocks, second_block, axis=1).astype(jnp.float32)
        partial_tiles = jnp.einsum('rgi,rgj->gij', weighted_cols, plain_cols)
        partial_tiles = partial_tiles * live_mask[:, None, None]
        return (raw_tiles.at[pair_ids].add(partial_tiles), None)
    start = jnp.zeros((PAIRS, BLOCK, BLOCK), jnp.float32)
    raw_tiles, _ = lax.scan(one_device, start, jnp.arange(device_total, dtype=jnp.int32))
    squares = lax.optimization_barrier(jnp.sum(jnp.square(matrix.astype(jnp.float32)), axis=0))
    root_mean = jnp.sqrt(squares / ROWS_TOTAL + 1e-06).reshape(NB, BLOCK)
    left_scale = root_mean[pair_blocks[:, 0]]
    right_scale = root_mean[pair_blocks[:, 1]]
    return raw_tiles / (SAMP * left_scale[:, :, None] * right_scale[:, None, :])
```

```python
import functools

import jax
import jax.numpy as jnp
from jax import lax
from jax.experimental import pallas as pl
from jax.experimental.pallas import tpu as pltpu
from jax.sharding import PartitionSpec as P

MESH = pl.DeviceIdType.MESH
epsilon = 1e-06
ROWS = 320
PADDED = 384
COLS = 16384
BLOCKS = 128
SAMPLES = 256
SLOTS = 256
CHUNKS = 4
Y_LANES = 37
UNROLL = 8
GROUPS = 8
FIRST, SECOND, PLACE, DENSE, OWNED, SPARE = 0, 256, 512, 768, 2816, 2832
TABLE = 2840
SMALL_CAP = 192


def prep_kernel(
    all_lists_ref, all_counts_ref, counts_vmem_ref, blocks_ref, picked_ref,
    table_ref, mult_ref, fits_ref, turned_ref, lists_ref, counts_ref, sem,
):
    s = lax.axis_index("rows")
    g = lax.axis_index("grp")
    me = lax.rem(s, 16)
    near = pl.ds((s // 16) * 16, 16)
    copies = (
        pltpu.make_async_copy(all_lists_ref.at[near], lists_ref, sem.at[0]),
        pltpu.make_async_copy(all_counts_ref.at[near], counts_ref, sem.at[1]),
    )
    for copy in copies:
        copy.start()
    turned_ref[...] = picked_ref[0].T
    most = jnp.max(jnp.sum(counts_vmem_ref[...], axis=1, keepdims=True))
    fits_ref[0] = (most <= SMALL_CAP).astype(jnp.int32)
    rows = lax.broadcasted_iota(jnp.int32, (128, 128), 0)
    zero = jnp.zeros((128, 128), jnp.int32)

    def clear(j, total):
        table_ref[FIRST + j] = 0
        table_ref[SECOND + j] = 0
        for i in range(8):
            table_ref[DENSE + j * 8 + i] = 64
        row = turned_ref[pl.ds(j, 1), :]
        return total + jnp.where(row == rows, 1, 0)

    total = lax.fori_loop(0, SAMPLES, clear, zero, unroll=4)
    mult_ref[:, 0, 0:128] = total.astype(jnp.float32).T

    for copy in copies:
        copy.wait()

    def compact(t, carry):
        pos, second, third = carry
        for x in range(4):
            r = x * 16 + t
            count = counts_ref[me, r]
            count_in = counts_ref[t, x * 16 + me]
            for k in range(4):
                j = t * 16 + x * 4 + k
                pair = lists_ref[me, k, r]
                live = k < count
                table_ref[FIRST + pos] = blocks_ref[0, pair]
                table_ref[SECOND + pos] = blocks_ref[1, pair]
                table_ref[PLACE + x * 64 + t * 4 + k] = jnp.where(live, pos, 0)
                pos = jnp.where(live, jnp.minimum(pos + 1, SLOTS - 1), pos)
                local = lists_ref[t, k, x * 16 + me] - (x * 16 + me) * 32
                place = DENSE + (x * 32 + local) * 16 + t
                table_ref[jnp.where(k < count_in, place, SPARE)] = t * 4 + k
                row = turned_ref[pl.ds(j, 1), :]
                second = second + jnp.where(row == rows + 128, 1, 0)
                third = third + jnp.where(row == rows + 256, 1, 0)
        return pos, second, third

    _, second, third = lax.fori_loop(0, 16, compact, (jnp.int32(0), zero, zero))
    mult_ref[:, 0, 128:256] = second.astype(jnp.float32).T
    mult_ref[:, 0, 256:384] = third.astype(jnp.float32).T

    def owned(i, carry):
        pair = (s * 4 + g) * 8 + i
        table_ref[OWNED + 2 * i] = blocks_ref[0, pair]
        table_ref[OWNED + 2 * i + 1] = blocks_ref[1, pair]
        return carry

    lax.fori_loop(0, 8, owned, 0)


def main_kernel(n, table_ref, mult_ref, matrix_ref, raw_ref, square_ref, *scratch):
    half = n // 2
    names = iter(scratch)
    mat = next(names)
    tiles = next(names)
    r1p = [next(names) for _ in range(CHUNKS)]
    r1m = [next(names) for _ in range(CHUNKS)]
    r2p = [next(names) for _ in range(CHUNKS)]
    r2m = [next(names) for _ in range(CHUNKS)]
    zs = [next(names) for _ in range(CHUNKS)]
    zr = [[next(names) for _ in range(4)] for _ in range(CHUNKS)]
    dn = [next(names) for _ in range(CHUNKS)]
    x1p = [next(names) for _ in range(CHUNKS)]
    x1m = [next(names) for _ in range(CHUNKS)]
    x2p = [next(names) for _ in range(CHUNKS)]
    x2m = [next(names) for _ in range(CHUNKS)]
    fin = [next(names) for _ in range(CHUNKS)]
    gathered = next(names)
    sq, qy, q1, qx, q2, qz, g1, g2 = [next(names) for _ in range(8)]
    load_sem = next(names)
    ysend, yrecv = next(names), next(names)
    zsend, zrecv = next(names), next(names)
    xsend, xrecv = next(names), next(names)
    fsend, frecv = next(names), next(names)
    qsend, qrecv = next(names), next(names)

    s = lax.axis_index("rows")
    y = lax.axis_index("grp")
    x = s // 16
    me = lax.rem(s, 16)
    yp, ym, yo = lax.rem(y + 1, 4), lax.rem(y + 3, 4), lax.rem(y + 2, 4)
    xp, xm, xo = lax.rem(x + 1, 4), lax.rem(x + 3, 4), lax.rem(x + 2, 4)

    def at_y(o):
        return (s, lax.rem(y + o, 4))

    def at_x(o):
        return (lax.rem(x + o, 4) * 16 + me, y)

    def at_z(o):
        return (x * 16 + lax.rem(me + o, 16), y)

    def load(b, carry):
        cols = pl.ds(pl.multiple_of(b * 128, 128), 128)
        pltpu.make_async_copy(matrix_ref.at[:, cols], mat.at[b, pl.ds(0, ROWS)], load_sem).start()
        return carry

    lax.fori_loop(0, BLOCKS, load, 0)

    barrier = pltpu.get_barrier_semaphore()
    for o in range(1, 4):
        pl.semaphore_signal(barrier, inc=1, device_id=at_y(o), device_id_type=MESH)
        pl.semaphore_signal(barrier, inc=1, device_id=at_x(o), device_id_type=MESH)
    for o in range(1, 16):
        pl.semaphore_signal(barrier, inc=1, device_id=at_z(o), device_id_type=MESH)

    def clear(b, carry):
        mat[b, pl.ds(ROWS, PADDED - ROWS)] = jnp.zeros((PADDED - ROWS, 128), jnp.bfloat16)
        return carry

    lax.fori_loop(0, BLOCKS, clear, 0, unroll=4)
    for u in range(CHUNKS):
        for step in range(4):
            zr[u][step][64] = jnp.zeros((8, 128), jnp.float32)
    whole = mat.at[:, pl.ds(0, ROWS)]
    pltpu.make_async_copy(whole, whole, load_sem).wait()

    def tile(j, carry):
        b = table_ref[FIRST + j]
        c = table_ref[SECOND + j]
        left = mat[b].T
        right = mat[c]
        weight = mult_ref[b]
        weighted = left * weight.astype(jnp.bfloat16)
        out = jnp.dot(weighted, right, preferred_element_type=jnp.float32)
        tiles[:, j] = out.reshape(16, 8, 128)
        return carry

    lanes = iter(range(Y_LANES))

    def y_copies(u, quarter, sources, target, o):
        copies = []
        for start, size, shift in sources:
            lane = next(lanes)
            copies.append(
                pltpu.make_async_remote_copy(
                    src_ref=tiles.at[quarter * CHUNKS + u, pl.ds(start, size)],
                    dst_ref=target.at[pl.ds(start - shift, size)],
                    send_sem=ysend.at[lane],
                    recv_sem=yrecv.at[lane],
                    device_id=at_y(o),
                    device_id_type=MESH,
                )
            )
        return copies

    group_size = n // GROUPS
    split = GROUPS // 2
    first_up, first_down, plain_up, plain_down, summed_up, summed_down = [], [], [], [], [], []
    for u in range(CHUNKS):
        count = split if u == 0 else 1
        size = half // count
        low = [(i * size, size, 0) for i in range(count)]
        high = [(half + i * size, size, 0) for i in range(count)]
        high_moved = [(start, size, half) for start, size, _ in high]
        if u == 1:
            high_moved = [(half, half // 2, half), (half + half // 2, half // 2, half)]
        first_up.append(y_copies(u, yo, low, r1p[u], 1))
        first_down.append(y_copies(u, yo, high_moved, r1m[u], 3))
        plain_up.append(y_copies(u, yp, high, r2p[u], 1))
        plain_down.append(y_copies(u, ym, low, r2m[u], 3))
        summed_up.append(y_copies(u, yp, [(0, half, 0)], r2p[u], 1))
        summed_down.append(y_copies(u, ym, [(half, half, 0)], r2m[u], 3))
    every_y = [c for kind in (first_up, first_down, plain_up, plain_down, summed_up, summed_down) for part in kind for c in part]

    def begin(*copies):
        for copy in copies:
            copy.start()

    def tiles_of(group):
        lax.fori_loop(group * group_size, (group + 1) * group_size, tile, 0, unroll=UNROLL)

    def add_up(u):
        for copy in first_up[u]:
            copy.wait_recv()

        def body(i, carry):
            tiles[yp * CHUNKS + u, i] = tiles[yp * CHUNKS + u, i] + r1p[u][i]
            return carry

        lax.fori_loop(0, half, body, 0, unroll=8)
        begin(*summed_up[u])

    def add_down(u):
        for copy in first_down[u]:
            copy.wait_recv()

        def body(i, carry):
            tiles[ym * CHUNKS + u, half + i] = tiles[ym * CHUNKS + u, half + i] + r1m[u][i]
            return carry

        lax.fori_loop(0, half, body, 0, unroll=8)
        begin(*summed_down[u])

    tiles_of(0)
    pl.semaphore_wait(barrier, 21)
    begin(first_up[0][0], plain_down[0][0])
    for i in range(1, split):
        tiles_of(i)
        begin(first_up[0][i], plain_down[0][i])
    for i in range(split):
        tiles_of(split + i)
        begin(first_down[0][i], plain_up[0][i])
        if i == split - 2:
            add_up(0)
    begin(first_down[1][0], *first_up[1])

    def squares(i, carry):
        for part in range(8):
            b = i * 8 + part

            def step(r, total):
                v = mat[b, pl.ds(pl.multiple_of(r * 32, 32), 32)].astype(jnp.float32)
                return total + v * v

            total = lax.fori_loop(0, ROWS // 32, step, jnp.zeros((32, 128), jnp.float32), unroll=True)
            sq[i, pl.ds(part, 1), :] = jnp.sum(total, axis=0, keepdims=True)
        return carry

    lax.fori_loop(0, 16, squares, 0)

    def q_copy(step, src, dst, device):
        return pltpu.make_async_remote_copy(
            src_ref=src,
            dst_ref=dst,
            send_sem=qsend.at[step],
            recv_sem=qrecv.at[step],
            device_id=device,
            device_id_type=MESH,
        )

    def q_wait(step, ref):
        pltpu.make_async_copy(ref, ref, qrecv.at[step]).wait()

    for o in range(1, 4):
        q_copy(0, sq.at[pl.ds(lax.rem(y + o, 4) * 4, 4)], qy.at[o - 1], at_y(o)).start()

    def z_send(u):
        for kind in (plain_up, plain_down, summed_up, summed_down):
            for copy in kind[u]:
                copy.wait_recv()

        for step, block in enumerate((xo, xp, xm, x)):

            def gather(i, carry, step=step, block=block):
                place = table_ref[PLACE + block * 64 + i]
                zs[u][step * 64 + i] = tiles[y * CHUNKS + u, place] + r2p[u][place] + r2m[u][place]
                return carry

            lax.fori_loop(0, 64, gather, 0, unroll=8)

            def send(o, carry, step=step):
                there = lax.rem(me + o, 16)
                pltpu.make_async_remote_copy(
                    src_ref=zs[u].at[pl.ds(step * 64 + there * 4, 4)],
                    dst_ref=zr[u][step].at[pl.ds(me * 4, 4)],
                    send_sem=zsend.at[u, step],
                    recv_sem=zrecv.at[u, step],
                    device_id=at_z(o),
                    device_id_type=MESH,
                ).start()
                return carry

            lax.fori_loop(1, 16, send, 0)
            zr[u][step][pl.ds(me * 4, 4)] = zs[u][pl.ds(step * 64 + me * 4, 4)]

    def x_copy(u, lane, src, dst, o):
        return pltpu.make_async_remote_copy(
            src_ref=src,
            dst_ref=dst,
            send_sem=xsend.at[u, lane],
            recv_sem=xrecv.at[u, lane],
            device_id=at_x(o),
            device_id_type=MESH,
        )

    x_copies = []
    for u in range(CHUNKS):
        x_copies.append(
            (
                x_copy(u, 0, dn[u].at[pl.ds(xo * 32, 16)], x1p[u], 1),
                x_copy(u, 1, dn[u].at[pl.ds(xo * 32 + 16, 16)], x1m[u], 3),
                x_copy(u, 2, dn[u].at[pl.ds(xp * 32, 32)], x2p[u], 1),
                x_copy(u, 3, dn[u].at[pl.ds(xm * 32, 32)], x2m[u], 3),
            )
        )

    blocks = (xo, xp, xm, x)

    def dense(u, step):
        landed = zs[u].at[pl.ds(0, 60)]
        pltpu.make_async_copy(landed, landed, zrecv.at[u, step]).wait()
        block = blocks[step]

        def body(i, carry):
            p = block * 32 + i
            parts = [zr[u][step][table_ref[DENSE + p * 16 + src]] for src in range(16)]
            while len(parts) > 1:
                parts = [a + b for a, b in zip(parts[::2], parts[1::2])]
            dn[u][p] = parts[0]
            return carry

        lax.fori_loop(0, 32, body, 0, unroll=2)

    def z_finish(u):
        dense(u, 0)
        begin(x_copies[u][0], x_copies[u][1])
        for step in (1, 2, 3):
            dense(u, step)

    def x_second(u):
        x_copies[u][0].wait_recv()
        x_copies[u][1].wait_recv()
        up, down = pl.ds(xp * 32, 16), pl.ds(xm * 32 + 16, 16)
        dn[u][up] = dn[u][up] + x1p[u][...]
        dn[u][down] = dn[u][down] + x1m[u][...]
        x_copies[u][2].start()
        x_copies[u][3].start()

    def x_finish(u):
        x_copies[u][2].wait_recv()
        x_copies[u][3].wait_recv()
        fin[u][...] = dn[u][pl.ds(x * 32, 32)] + x2p[u][...] + x2m[u][...]
        for o in range(1, 4):
            pltpu.make_async_remote_copy(
                src_ref=fin[u].at[pl.ds(lax.rem(y + o, 4) * 8, 8)],
                dst_ref=gathered.at[y * CHUNKS + u],
                send_sem=fsend.at[u],
                recv_sem=frecv.at[u],
                device_id=at_y(o),
                device_id_type=MESH,
            ).start()
        gathered[y * CHUNKS + u] = fin[u][pl.ds(y * 8, 8)]

    add_down(0)
    begin(first_down[1][1], *plain_up[1], *plain_down[1])
    z_send(0)
    q_wait(0, qy)
    q1[...] = sq[pl.ds(y * 4, 4)] + qy[0] + qy[1] + qy[2]
    for o in range(1, 4):
        q_copy(1, q1.at[lax.rem(x + o, 4)], qx.at[o - 1], at_x(o)).start()
    add_up(1)
    add_down(1)
    begin(*first_up[2], *first_down[2], *plain_up[2], *plain_down[2])
    q_wait(1, qx)
    q2[...] = q1[x] + qx[0] + qx[1] + qx[2]
    for o in range(1, 16):
        q_copy(2, q2, qz.at[o - 1], at_z(o)).start()
    z_send(1)
    z_finish(0)
    add_up(2)
    add_down(2)
    begin(*first_up[3], *first_down[3], *plain_up[3], *plain_down[3])
    q_wait(2, qz)
    total = q2[...]
    for o in range(15):
        total = total + qz[o]
    g1[x] = total
    for o in range(1, 4):
        q_copy(3, g1.at[x], g1.at[x], at_x(o)).start()
    z_send(2)
    z_finish(1)
    add_up(3)
    add_down(3)
    x_second(0)
    pltpu.make_async_copy(g1.at[pl.ds(0, 3)], g1.at[pl.ds(0, 3)], qrecv.at[3]).wait()
    for o in range(1, 4):
        q_copy(4, g1, g2.at[pl.ds(y * 4, 4)], at_y(o)).start()
    g2[pl.ds(y * 4, 4)] = g1[...]
    z_send(3)
    x_finish(0)
    z_finish(2)
    x_second(1)
    x_finish(1)
    x_second(2)
    x_finish(2)
    dense(3, 0)
    begin(x_copies[3][0], x_copies[3][1])
    dense(3, 1)
    dense(3, 2)
    x_second(3)
    dense(3, 3)
    x_finish(3)

    pltpu.make_async_copy(g2.at[pl.ds(0, 12)], g2.at[pl.ds(0, 12)], qrecv.at[4]).wait()
    square_ref[...] = g2[...]
    for u in range(CHUNKS):
        piece = gathered.at[pl.ds(0, 3)]
        pltpu.make_async_copy(piece, piece, frecv.at[u]).wait()
    raw_ref[...] = gathered[...]

    for copy in every_y:
        copy.wait_send()
    for u in range(CHUNKS):
        for step in range(4):
            piece = zs[u].at[pl.ds(0, 60)]
            pltpu.make_async_copy(piece, piece, zsend.at[u, step]).wait()
        for copy in x_copies[u]:
            copy.wait_send()
        piece = fin[u].at[pl.ds(0, 24)]
        pltpu.make_async_copy(piece, piece, fsend.at[u]).wait()
    for step, ref in ((0, qy), (1, qx), (2, qz), (3, g1.at[pl.ds(0, 3)]), (4, g2.at[pl.ds(0, 12)])):
        pltpu.make_async_copy(ref, ref, qsend.at[step]).wait()


def finish_kernel(table_ref, raw_ref, square_ref, out_ref, scale_ref):
    scale_ref[...] = jnp.sqrt(square_ref[...] / (ROWS * 256) + epsilon)
    for p in range(8):
        b = table_ref[OWNED + 2 * p]
        c = table_ref[OWNED + 2 * p + 1]
        left = jnp.broadcast_to(scale_ref[pl.ds(b, 1), :], (128, 128)).T
        right = scale_ref[pl.ds(c, 1), :]
        value = raw_ref[:, p].reshape(128, 128)
        out_ref[p] = value / (SAMPLES * left * right)


def vmem():
    return pl.BlockSpec(memory_space=pltpu.VMEM)


def smem():
    return pl.BlockSpec(memory_space=pltpu.SMEM)


def main_call(n, collective, table, mult, matrix):
    half = n // 2

    def tile_buffer(*lead):
        return pltpu.VMEM((*lead, 8, 128), jnp.float32)

    scratch = [pltpu.VMEM((BLOCKS, PADDED, 128), jnp.bfloat16), tile_buffer(16, n)]
    for shape in ((half,), (half,), (n,), (n,), (SLOTS,)):
        scratch += [tile_buffer(*shape) for _ in range(CHUNKS)]
    scratch += [tile_buffer(65) for _ in range(CHUNKS * 4)]
    for shape in ((128,), (16,), (16,), (32,), (32,), (32,)):
        scratch += [tile_buffer(*shape) for _ in range(CHUNKS)]
    scratch += [tile_buffer(16, 8)]
    scratch += [tile_buffer(16), tile_buffer(3, 4), tile_buffer(4), tile_buffer(3)]
    scratch += [tile_buffer(), tile_buffer(15), tile_buffer(4), tile_buffer(16)]
    dma = pltpu.SemaphoreType.DMA
    scratch += [dma]
    for shape in ((Y_LANES,), (CHUNKS, 4), (CHUNKS, 4), (CHUNKS,), (5,)):
        scratch += [dma(shape), dma(shape)]
    return pl.pallas_call(
        functools.partial(main_kernel, n),
        out_shape=(
            jax.ShapeDtypeStruct((16, 8, 8, 128), jnp.float32),
            jax.ShapeDtypeStruct((16, 8, 128), jnp.float32),
        ),
        in_specs=[smem(), vmem(), pl.BlockSpec(memory_space=pl.ANY)],
        out_specs=(vmem(), vmem()),
        scratch_shapes=scratch,
        compiler_params=pltpu.CompilerParams(
            collective_id=collective, has_side_effects=True, vmem_limit_bytes=67043328
        ),
        name=f"tiles_{n}",
    )(table, mult, matrix)


def shards(matrix, sample_rows, pair_list, pair_count, pair_blocks):
    table, mult, fits = pl.pallas_call(
        prep_kernel,
        out_shape=(
            jax.ShapeDtypeStruct((TABLE,), jnp.int32),
            jax.ShapeDtypeStruct((BLOCKS, 1, PADDED), jnp.float32),
            jax.ShapeDtypeStruct((1,), jnp.int32),
        ),
        in_specs=[pl.BlockSpec(memory_space=pl.ANY)] * 2 + [vmem(), smem(), vmem()],
        out_specs=(smem(), vmem(), smem()),
        scratch_shapes=[
            pltpu.VMEM((SAMPLES, BLOCKS), jnp.int32),
            pltpu.SMEM((16, 4, 64), jnp.int32),
            pltpu.SMEM((16, 64), jnp.int32),
            pltpu.SemaphoreType.DMA((2,)),
        ],
        name="prep",
    )(jnp.swapaxes(pair_list, 1, 2), pair_count, pair_count, pair_blocks.T, sample_rows)
    raw, square = lax.cond(
        fits[0] > 0,
        functools.partial(main_call, SMALL_CAP, 1),
        functools.partial(main_call, SLOTS, 2),
        table,
        mult,
        matrix,
    )
    return pl.pallas_call(
        finish_kernel,
        out_shape=jax.ShapeDtypeStruct((8, 128, 128), jnp.float32),
        in_specs=[smem(), vmem(), vmem()],
        out_specs=vmem(),
        scratch_shapes=[pltpu.VMEM((BLOCKS, 128), jnp.float32)],
        name="finish",
    )(table, raw, square.reshape(BLOCKS, 128))


def solution(mesh):
    in_specs = (P(("rows", "grp"), None), P(("rows", "grp"), None, None), P(), P(), P())
    out_specs = P(("rows", "grp"), None, None)
    return jax.shard_map(shards, mesh=mesh, in_specs=in_specs, out_specs=out_specs, check_vma=False)
```
